8 devices in a mesh: dp: 2 (over z, y), tp: 4 (over x, core).
Axes of the slice: x: 2, y: 2, z: 1, core: 2. Of those that a mesh axis runs over, the one named last changes fastest.
Arguments:
- x_norm: bfloat16 [4096, 3072], P(('dp', 'tp')), parts along dimension 0
- grad_y: bfloat16 [4096, 3072], P(('dp', 'tp')), parts along dimension 0
- u_gate: bfloat16 [4096, 8192], P('dp', 'tp'), parts along dimension 0
- u_up: bfloat16 [4096, 8192], P('dp', 'tp'), parts along dimension 0
- w_gate: bfloat16 [3072, 8192], P(None, 'tp')
- w_up: bfloat16 [3072, 8192], P(None, 'tp')
- w_down: bfloat16 [8192, 3072], P('tp')
- x_in: bfloat16 [4096, 3072], P(('dp', 'tp')), parts along dimension 0
- gamma: bfloat16 [3072], replicated
- grad_res: bfloat16 [4096, 3072], P(('dp', 'tp')), parts along dimension 0
- attn_out: bfloat16 [4096, 3072], P('dp', 'tp'), parts along dimension 0
- w_out: bfloat16 [3072, 3072], P('tp')
Outputs:
- output 1: bfloat16 [4096, 3072], P(('dp', 'tp')), parts along dimension 0
- output 2: bfloat16 [4096, 3072], P('dp', 'tp'), parts along dimension 0
- output 3: float32 [6144, 8192], P('dp', 'tp'), parts along dimension 0
- output 4: float32 [6144, 8192], P('dp', 'tp'), parts along dimension 0
- output 5: float32 [16384, 3072], P(('dp', 'tp')), parts along dimension 0
- output 6: float32 [6144, 3072], P(('dp', 'tp')), parts along dimension 0
There are 2 independent parts. The reference program is written for one: setup_inputs(seed, part) draws one part's arguments, and reference() takes and returns one part's arrays. A program takes and returns all parts, laid end to end along the dimension named above; an argument that names none is the same for every part.
All inputs are finite; a program needn't handle non-finite values.
Results may differ from the reference program's by a relative error of at most 0.0124445.
Values are sent between devices in bfloat16 or wider.
A program may use at most 1 GiB of HBM per device.

```python
import jax
import jax.numpy as jnp
from jax import lax

HIDDEN = 3072
FFN_DIM = 8192
TOKENS = 2048
NORM_EPS = 1e-5


def setup_inputs(seed: int = 0, part: int = 0) -> dict:
    part_keys = jax.random.split(jax.random.fold_in(jax.random.key(seed), part), 7)
    weight_keys = jax.random.split(jax.random.key(seed + 1), 5)
    xin_keys = jax.random.split(part_keys[4], 2)
    act_shape = (TOKENS, HIDDEN)
    ffn_shape = (TOKENS, FFN_DIM)
    x_norm = jax.random.normal(part_keys[0], act_shape, jnp.float32)
    grad_y = jax.random.normal(part_keys[1], act_shape, jnp.float32)
    u_gate = jax.random.normal(part_keys[2], ffn_shape, jnp.float32)
    u_up = jax.random.normal(part_keys[3], ffn_shape, jnp.float32)
    xin_scale = jnp.exp(jax.random.uniform(xin_keys[0], (TOKENS, 1), jnp.float32, -1.0, 1.0))
    x_in = jax.random.normal(xin_keys[1], act_shape, jnp.float32) * xin_scale
    grad_res = 0.5 * jax.random.normal(part_keys[5], act_shape, jnp.float32)
    attn_out = jax.random.normal(part_keys[6], act_shape, jnp.float32)
    w_gate = jax.random.normal(weight_keys[0], (HIDDEN, FFN_DIM), jnp.float32) * HIDDEN ** -0.5
    w_up = jax.random.normal(weight_keys[1], (HIDDEN, FFN_DIM), jnp.float32) * HIDDEN ** -0.5
    w_down = jax.random.normal(weight_keys[2], (FFN_DIM, HIDDEN), jnp.float32) * FFN_DIM ** -0.5
    w_out = jax.random.normal(weight_keys[3], (HIDDEN, HIDDEN), jnp.float32) * HIDDEN ** -0.5
    gamma = 1.0 + 0.3 * jax.random.normal(weight_keys[4], (HIDDEN,), jnp.float32)
    return dict(
        x_norm=x_norm.astype(jnp.bfloat16),
        grad_y=grad_y.astype(jnp.bfloat16),
        u_gate=u_gate.astype(jnp.bfloat16),
        u_up=u_up.astype(jnp.bfloat16),
        w_gate=w_gate.astype(jnp.bfloat16),
        w_up=w_up.astype(jnp.bfloat16),
        w_down=w_down.astype(jnp.bfloat16),
        x_in=x_in.astype(jnp.bfloat16),
        gamma=gamma.astype(jnp.bfloat16),
        grad_res=grad_res.astype(jnp.bfloat16),
        attn_out=attn_out.astype(jnp.bfloat16),
        w_out=w_out.astype(jnp.bfloat16),
    )


def reference(x_norm, grad_y, u_gate, u_up, w_gate, w_up, w_down, x_in, gamma, grad_res, attn_out, w_out):
    gate_f = u_gate.astype(jnp.float32)
    up_f = u_up.astype(jnp.float32)
    sig_gate = jax.nn.sigmoid(gate_f)
    act_gate = gate_f * sig_gate
    silu_grad = sig_gate * (1.0 + gate_f * (1.0 - sig_gate))
    hidden_z = (act_gate * up_f).astype(jnp.bfloat16)
    gw_down = jnp.dot(hidden_z.T, grad_y, preferred_element_type=jnp.float32)
    grad_h = jnp.dot(grad_y, w_down.T, preferred_element_type=jnp.float32)
    grad_up = (grad_h * act_gate).astype(jnp.bfloat16)
    grad_gate = (grad_h * up_f * silu_grad).astype(jnp.bfloat16)
    grad_x = (jnp.dot(grad_gate, w_gate.T, preferred_element_type=jnp.float32)
              + jnp.dot(grad_up, w_up.T, preferred_element_type=jnp.float32)).astype(jnp.bfloat16)
    gw_gate = jnp.dot(x_norm.T, grad_gate, preferred_element_type=jnp.float32)
    gw_up = jnp.dot(x_norm.T, grad_up, preferred_element_type=jnp.float32)
    xin_f = x_in.astype(jnp.float32)
    inv_rms = lax.rsqrt(jnp.mean(xin_f * xin_f, axis=-1, keepdims=True) + NORM_EPS)
    scaled = grad_x.astype(jnp.float32) * gamma.astype(jnp.float32)
    proj_mean = jnp.mean(scaled * xin_f, axis=-1, keepdims=True)
    grad_sum = (grad_res.astype(jnp.float32)
                + inv_rms * (scaled - xin_f * (inv_rms * inv_rms) * proj_mean)).astype(jnp.bfloat16)
    grad_attn = jnp.dot(grad_sum, w_out.T, preferred_element_type=jnp.float32).astype(jnp.bfloat16)
    gw_out = jnp.dot(attn_out.T, grad_sum, preferred_element_type=jnp.float32)
    return grad_sum, grad_attn, gw_gate, gw_up, gw_down, gw_out
```

```python
import functools

import jax
import jax.numpy as jnp
from jax import lax
from jax.experimental import pallas as pl
from jax.experimental.pallas import tpu as pltpu
from jax.sharding import PartitionSpec as P


NORM_EPS = 1e-5
F32 = jnp.float32
BF16 = jnp.bfloat16
NT = (((1,), (1,)), ((), ()))
TN = (((0,), (0,)), ((), ()))
VMEM_LIMIT = 67043328


def call(kernel, grid, in_specs, out_specs, out_shape, flops, nbytes, scratch=(), after=(), offs=None, aliases=None, keep_offs=False):
    n_in, n_after = len(in_specs), len(after)
    n_pre = 0 if offs is None else 1

    def body(*refs):
        pre, refs = refs[:n_pre], refs[n_pre:]
        kernel(*(pre if keep_offs else ()), *refs[:n_in], *refs[n_in + n_after:])

    def run(*args):
        pre = () if offs is None else (offs,)
        return launch(pre, args)

    def launch(pre, args):
        return pl.pallas_call(
            body,
            grid_spec=pltpu.PrefetchScalarGridSpec(
                num_scalar_prefetch=n_pre,
                grid=grid,
                in_specs=list(in_specs) + [pl.BlockSpec(memory_space=pl.ANY)] * n_after,
                out_specs=out_specs,
                scratch_shapes=list(scratch),
            ),
            out_shape=out_shape,
            input_output_aliases={n_pre + i: o for i, o in (aliases or {}).items()},
            compiler_params=pltpu.CompilerParams(
                vmem_limit_bytes=VMEM_LIMIT, dimension_semantics=("arbitrary",) * len(grid)
            ),
            cost_estimate=pl.CostEstimate(flops=flops, bytes_accessed=nbytes, transcendentals=0),
        )(*pre, *args, *after)

    return run


def input_grads(pieces, starts, w_down, w_gate, w_up, u_gate, u_up, offs, cols, x_cols, after=()):
    rows, width = pieces[0].shape
    n_cols = w_down.shape[0]
    total = 2 * rows
    n_gate, n_x = n_cols // cols, width // x_cols

    def kernel(y0, y1, wd, g0, g1, u0, u1, wg, wu, o_gate, o_up, o_z, o_x0, o_x1, s_gate, s_up):
        step = pl.program_id(0)

        @pl.when(step < n_gate)
        def _():
            at = pl.ds(pl.multiple_of(step * cols, cols), cols)
            grad_y = jnp.concatenate([y0[...], y1[...]], axis=0)
            grad_h = lax.dot_general(grad_y, wd[...], NT, preferred_element_type=F32)
            gate_f = jnp.concatenate([g0[...], g1[...]], axis=0).astype(F32)
            up_f = jnp.concatenate([u0[...], u1[...]], axis=0).astype(F32)
            sig = jax.nn.sigmoid(gate_f)
            act = gate_f * sig
            d_up = (grad_h * act).astype(BF16)
            d_gate = (grad_h * up_f * (sig * (1.0 + gate_f * (1.0 - sig)))).astype(BF16)
            o_z[...] = (act * up_f).astype(BF16)
            o_up[...] = d_up
            o_gate[...] = d_gate
            s_up[:, at] = d_up
            s_gate[:, at] = d_gate

        @pl.when(step >= n_gate)
        def _():
            part = (lax.dot_general(s_gate[...], wg[...], NT, preferred_element_type=F32)
                    + lax.dot_general(s_up[...], wu[...], NT, preferred_element_type=F32)).astype(BF16)
            o_x0[...] = part[:rows]
            o_x1[...] = part[rows:]

    first = lambda j: jnp.minimum(j, n_gate - 1)
    second = lambda j: jnp.maximum(j - n_gate, 0)
    whole = pl.BlockSpec((rows, width), lambda j, o: (0, 0))
    tiles = [pl.BlockSpec((rows, cols), functools.partial(lambda s, j, o: (s(o), first(j)), s)) for s in starts]
    w_x = pl.BlockSpec((x_cols, n_cols), lambda j, o: (second(j), 0))
    out = pl.BlockSpec((total, cols), lambda j, o: (0, first(j)))
    out_x = pl.BlockSpec((rows, x_cols), lambda j, o: (0, second(j)))
    return call(
        kernel, (n_gate + n_x,),
        [whole, whole, pl.BlockSpec((cols, width), lambda j, o: (first(j), 0)), *tiles, *tiles, w_x, w_x],
        [out] * 3 + [out_x] * 2,
        [jax.ShapeDtypeStruct((total, n_cols), BF16)] * 3 + [jax.ShapeDtypeStruct((rows, width), BF16)] * 2,
        6 * total * width * n_cols, 2 * n_cols * (3 * width + 5 * total),
        scratch=[pltpu.VMEM((total, n_cols), BF16)] * 2, after=after, offs=offs,
    )(*pieces, w_down, u_gate, u_gate, u_up, u_up, w_gate, w_up)


def gw_in(x_parts, gates, ups, span, prev, rows, cols, after=()):
    width = x_parts[0].shape[1]
    n_tok = sum(x.shape[0] for x in x_parts)
    n_cols = gates[0].shape[1]
    half = gates[1].shape[0] // 2
    start, count = span[0] // rows, (span[1] - span[0]) // rows

    def kernel(*refs):
        x_own, x_par, x_acr, x_dia = (r[...] for r in refs[:4])
        x = [jnp.concatenate([x_own, x_par], axis=0)]
        x += [jnp.concatenate([x_acr[c * half:(c + 1) * half], x_dia[c * half:(c + 1) * half]], axis=0) for c in range(2)]
        for ds, out in ((refs[4:7], refs[-2]), (refs[7:10], refs[-1])):
            total = None
            for a, d in zip(x, ds):
                term = lax.dot_general(a, d[...], TN, preferred_element_type=F32)
                total = term if total is None else total + term
            out[...] = total

    in_specs = [pl.BlockSpec((x.shape[0], rows), lambda i, j: (0, start + i)) for x in x_parts]
    in_specs += [pl.BlockSpec((d.shape[0], cols), lambda i, j: (0, j)) for d in (*gates, *ups)]
    args = [*x_parts, *gates, *ups]
    aliases = None
    if prev is not None:
        in_specs += [pl.BlockSpec(memory_space=pl.ANY)] * 2
        args += list(prev)
        aliases = {10: 0, 11: 1}
    return call(
        kernel, (count, n_cols // cols), in_specs,
        [pl.BlockSpec((rows, cols), lambda i, j: (start + i, j))] * 2,
        [jax.ShapeDtypeStruct((width, n_cols), F32)] * 2,
        4 * n_tok * (span[1] - span[0]) * n_cols, 8 * (span[1] - span[0]) * n_cols, after=after, aliases=aliases,
    )(*args)


def gw_down(zs, y_pairs, rows, cols, after=()):
    n_rows = zs[0].shape[1]
    width = y_pairs[0][0].shape[1]
    flat = [y for pair in y_pairs for y in pair]
    n_tok = sum(z.shape[0] for z in zs)

    def kernel(z0, z1, z2, a0, b0, a1, b1, a2, b2, out):
        total = None
        for z, a, b in ((z0, a0, b0), (z1, a1, b1), (z2, a2, b2)):
            y = jnp.concatenate([a[...], b[...]], axis=0)
            term = lax.dot_general(z[...], y, TN, preferred_element_type=F32)
            total = term if total is None else total + term
        out[...] = total

    return call(
        kernel, (n_rows // rows, width // cols),
        [pl.BlockSpec((z.shape[0], rows), lambda i, j: (0, i)) for z in zs]
        + [pl.BlockSpec((y.shape[0], cols), lambda i, j: (0, j)) for y in flat],
        pl.BlockSpec((rows, cols), lambda i, j: (i, j)),
        jax.ShapeDtypeStruct((n_rows, width), F32),
        2 * n_tok * width * n_rows, 4 * width * n_rows, after=after,
    )(*zs, *flat)


def head_rows(x, start, rows, block=128, after=()):
    width = x.shape[1]
    first = start // block

    def kernel(src, out):
        out[...] = src[...]

    return call(
        kernel, (rows // block,), [pl.BlockSpec((block, width), lambda i: (first + i, 0))],
        pl.BlockSpec((block, width), lambda i: (i, 0)), jax.ShapeDtypeStruct((rows, width), x.dtype),
        rows * width, rows * width * 4, after=after,
    )(x)


def norm_chunk(parts, starts, rows, first_row, x_in, gamma, grad_res, prev, cuts, block=128, after=()):
    width = x_in.shape[1]
    n_cuts = len(cuts)
    edges = [sum(cuts[:k]) // block for k in range(n_cuts + 1)]

    def kernel(p0, p1, p2, xin, gam, res, *outs):
        outs = outs[-1 - n_cuts:]
        grad_x = (p0[...].astype(F32) + p1[...].astype(F32) + p2[...].astype(F32)).astype(BF16).astype(F32)
        xin_f = xin[...].astype(F32)
        inv_rms = lax.rsqrt(jnp.mean(xin_f * xin_f, axis=-1, keepdims=True) + NORM_EPS)
        scaled = grad_x * gam[...].astype(F32)
        proj_mean = jnp.mean(scaled * xin_f, axis=-1, keepdims=True)
        out = (res[...].astype(F32) + inv_rms * (scaled - xin_f * (inv_rms * inv_rms) * proj_mean)).astype(BF16)
        outs[-1][...] = out
        for k in range(n_cuts):
            @pl.when((pl.program_id(0) >= edges[k]) & (pl.program_id(0) < edges[k + 1]))
            def _(k=k):
                outs[k][...] = out

    first = first_row // block
    at = lambda s: pl.BlockSpec((block, width), lambda i: (s + i, 0))
    cut = lambda k: pl.BlockSpec((block, width), lambda i: (jnp.clip(i - edges[k], 0, edges[k + 1] - edges[k] - 1), 0))
    in_specs = [at(s // block) for s in starts] + [at(first), pl.BlockSpec((1, width), lambda i: (0, 0)), at(first)]
    args = [*parts, x_in, gamma, grad_res]
    aliases = None
    if prev is not None:
        in_specs.append(pl.BlockSpec(memory_space=pl.ANY))
        args.append(prev)
        aliases = {len(in_specs) - 1: n_cuts}
    return call(
        kernel, (rows // block,), in_specs, [cut(k) for k in range(n_cuts)] + [at(first)],
        [jax.ShapeDtypeStruct((c, width), BF16) for c in cuts] + [jax.ShapeDtypeStruct(x_in.shape, BF16)],
        rows * width * 20, rows * width * 14, after=after, aliases=aliases,
    )(*args)


def grad_attention(pieces, at_rows, blocks, w_out, offs, n_tok, after=()):
    n_cols, width = w_out.shape
    n = len(pieces)
    size = n_tok // 8

    def kernel(*refs):
        srcs, w, out = refs[:n], refs[n], refs[-1]
        for q in range(n):
            @pl.when(pl.program_id(0) == q)
            def _(q=q):
                out[...] = lax.dot_general(srcs[q][...], w[...], NT, preferred_element_type=F32).astype(BF16)

    def out_map(j, o):
        row = blocks[0](o)
        for q in range(1, n):
            row = jnp.where(j >= q, blocks[q](o), row)
        return (row, 0)

    return call(
        kernel, (n,),
        [pl.BlockSpec((size, width), functools.partial(lambda r, j, o: (r, 0), r)) for r in at_rows]
        + [pl.BlockSpec((n_cols, width), lambda j, o: (0, 0))],
        pl.BlockSpec((size, n_cols), out_map), jax.ShapeDtypeStruct((n_tok, n_cols), BF16),
        2 * n * size * width * n_cols, 2 * width * n_cols, after=after, offs=offs,
    )(*pieces, w_out)


def out_grads(pieces, blocks, todo, attn_out, w_out, offs, d_attn, cols, after=()):
    n_tok, n_rows = attn_out.shape
    width = w_out.shape[1]
    n = len(pieces)
    sizes = [p.shape[0] for p in pieces]
    left = sum(sizes[q] for q in todo)
    last = width // cols - 1

    def kernel(offs_ref, *refs):
        srcs, attn, w = refs[:n], refs[n:2 * n], refs[2 * n]
        o_attn, o_w, acc, done, sem = refs[-5:]
        step = pl.program_id(0)
        term = lax.dot_general(jnp.concatenate([srcs[q][...] for q in todo], axis=0), w[...], NT, preferred_element_type=F32)
        lhs = jnp.concatenate([a[...] for a in attn], axis=0)
        rhs = jnp.concatenate([src[...] for src in srcs], axis=0)
        o_w[...] = lax.dot_general(lhs, rhs, TN, preferred_element_type=F32)

        @pl.when(step == 0)
        def _():
            acc[...] = term

        @pl.when((step > 0) & (step < last))
        def _():
            acc[...] += term

        @pl.when(step == last)
        def _():
            done[...] = (acc[...] + term).astype(BF16)
            copies, first = [], 0
            for k, q in enumerate(todo):
                row = pl.multiple_of(blocks[q](offs_ref) * sizes[q], sizes[q])
                copies.append(pltpu.make_async_copy(
                    done.at[pl.ds(first, sizes[q])], o_attn.at[pl.ds(row, sizes[q])], sem.at[k]))
                copies[-1].start()
                first += sizes[q]
            for copy in copies:
                copy.wait()

    in_specs = [pl.BlockSpec((r, cols), lambda j, o: (0, j)) for r in sizes]
    in_specs += [pl.BlockSpec((r, n_rows), functools.partial(lambda m, j, o: (m(o), 0), m)) for r, m in zip(sizes, blocks)]
    in_specs += [pl.BlockSpec((n_rows, cols), lambda j, o: (0, j)), pl.BlockSpec(memory_space=pl.ANY)]
    return call(
        kernel, (width // cols,), in_specs,
        [pl.BlockSpec(memory_space=pl.ANY), pl.BlockSpec((n_rows, cols), lambda j, o: (0, j))],
        [jax.ShapeDtypeStruct((n_tok, n_rows), BF16), jax.ShapeDtypeStruct((n_rows, width), F32)],
        2 * (n_tok + left) * width * n_rows, 4 * width * n_rows, after=after, offs=offs, keep_offs=True,
        aliases={2 * n + 1: 0},
        scratch=[pltpu.VMEM((left, n_rows), F32), pltpu.VMEM((left, n_rows), BF16), pltpu.SemaphoreType.DMA((len(todo),))],
    )(*pieces, *([attn_out] * n), w_out, d_attn)


def solution(mesh):
    token_spec = P(("dp", "tp"), None)
    split_cols = P("dp", "tp")
    weight_cols = P(None, "tp")
    weight_rows = P("tp", None)
    partner = [(i, i ^ 1) for i in range(4)]
    across = [(i, i ^ 2) for i in range(4)]

    def swap(x):
        return lax.ppermute(x, "tp", partner)

    def send(x):
        return lax.ppermute(x, "tp", across)

    def backward(x_norm, grad_y, u_gate, u_up, w_gate, w_up, w_down, x_in, gamma, grad_res, attn_out, w_out):
        own, width = grad_y.shape
        half = own // 2
        n_tok = u_gate.shape[0]
        offs = lax.axis_index("tp") ^ jnp.arange(4, dtype=jnp.int32)
        gain = gamma.reshape(1, width)
        of = lambda p, c: (lambda o: 2 * o[p] + c)
        weights = (w_down, w_gate, w_up, u_gate, u_up, offs)

        y_par = swap(grad_y)
        head0 = head_rows(grad_y, 0, half)
        head1 = head_rows(grad_y, half, half, after=(head0,))
        y_acr = [send(head0), send(head1)]
        y_dia = [swap(y_acr[c]) for c in range(2)]
        x_par = swap(x_norm)
        x_acr = send(x_norm)
        x_dia = swap(x_acr)
        x_parts = (x_norm, x_par, x_acr, x_dia)

        g_l, u_l, z_l, dx_own, dx_par = input_grads(
            (grad_y, y_par), (lambda o: o[0], lambda o: o[1]), *weights, 256, 512, after=(gain, head1))
        dx_sib = swap(dx_par)
        gates, ups, zs, dx_rem = [g_l], [u_l], [z_l], []
        last = dx_own
        for c in range(2):
            g, u, z, to_acr, to_dia = input_grads(
                (y_acr[c], y_dia[c]), (of(2, c), of(3, c)), *weights, 512, 512, after=(last,))
            dx_rem.append((to_acr, swap(to_dia)))
            last = to_acr
            gates.append(g)
            ups.append(u)
            zs.append(z)
        both = [(a.astype(F32) + b.astype(F32)).astype(BF16) for a, b in dx_rem]
        rs = [send(both[c]) for c in range(2)]

        gwd = gw_down(zs, ((grad_y, y_par), (y_acr[0], y_dia[0]), (y_acr[1], y_dia[1])), 1024, 512, after=(both[0],))
        third = width // 3
        norm = (x_in, gain, grad_res)
        gw = gw_in(x_parts, gates, ups, (0, third), None, 1024, 512, after=(gwd, both[1]))
        ds0, ds = norm_chunk((dx_own, dx_sib, rs[0]), (0, 0, 0), half, 0, *norm, None, (half,), after=(gw[0],))
        s_acr0, s_par0 = send(ds0), swap(ds0)
        gw = gw_in(x_parts, gates, ups, (third, 2 * third), gw, 1024, 512, after=(ds0,))
        ds1, ds = norm_chunk((dx_own, dx_sib, rs[1]), (half, half, 0), half, half, *norm, ds, (half,), after=(gw[0],))
        s_acr1, s_par1 = send(ds1), swap(ds1)
        gwg, gwu = gw_in(x_parts, gates, ups, (2 * third, width), gw, 1024, 512, after=(ds1,))
        s_dia0, s_dia1 = swap(s_acr0), swap(s_acr1)

        d_attn = grad_attention((ds, ds, s_par0, s_par1, s_acr0, s_dia0), (0, 1, 0, 0, 0, 0),
                                (of(0, 0), of(0, 1), of(1, 0), of(1, 1), of(2, 0), of(3, 0)), w_out, offs, n_tok, after=(gwg,))
        d_attn, gwo = out_grads((ds, s_par0, s_par1, s_acr0, s_dia0, s_acr1, s_dia1),
                                (lambda o: o[0], of(1, 0), of(1, 1), of(2, 0), of(3, 0), of(2, 1), of(3, 1)), (5, 6),
                                attn_out, w_out, offs, d_attn, 512)
        return ds, d_attn, gwg, gwu, gwd, gwo

    return jax.shard_map(
        backward,
        mesh=mesh,
        in_specs=(token_spec, token_spec, split_cols, split_cols, weight_cols, weight_cols, weight_rows,
                  token_spec, P(None), token_spec, split_cols, weight_rows),
        out_specs=(token_spec, split_cols, split_cols, split_cols, token_spec, token_spec),
        check_vma=False,
    )
```

```python
import functools

import jax
import jax.numpy as jnp
from jax import lax
from jax.experimental import pallas as pl
from jax.experimental.pallas import tpu as pltpu
from jax.sharding import PartitionSpec as P


NORM_EPS = 1e-5
F32 = jnp.float32
BF16 = jnp.bfloat16
NT = (((1,), (1,)), ((), ()))
TN = (((0,), (0,)), ((), ()))
VMEM_LIMIT = 67043328


def call(kernel, grid, in_specs, out_specs, out_shape, flops, nbytes, scratch=(), after=(), offs=None, aliases=None, keep_offs=False):
    n_in, n_after = len(in_specs), len(after)
    n_pre = 0 if offs is None else 1

    def body(*refs):
        pre, refs = refs[:n_pre], refs[n_pre:]
        kernel(*(pre if keep_offs else ()), *refs[:n_in], *refs[n_in + n_after:])

    def run(*args):
        pre = () if offs is None else (offs,)
        return launch(pre, args)

    def launch(pre, args):
        return pl.pallas_call(
            body,
            grid_spec=pltpu.PrefetchScalarGridSpec(
                num_scalar_prefetch=n_pre,
                grid=grid,
                in_specs=list(in_specs) + [pl.BlockSpec(memory_space=pl.ANY)] * n_after,
                out_specs=out_specs,
                scratch_shapes=list(scratch),
            ),
            out_shape=out_shape,
            input_output_aliases={n_pre + i: o for i, o in (aliases or {}).items()},
            compiler_params=pltpu.CompilerParams(
                vmem_limit_bytes=VMEM_LIMIT, dimension_semantics=("arbitrary",) * len(grid)
            ),
            cost_estimate=pl.CostEstimate(flops=flops, bytes_accessed=nbytes, transcendentals=0),
        )(*pre, *args, *after)

    return run


def input_grads(pieces, starts, w_down, w_gate, w_up, u_gate, u_up, offs, cols, x_cols, terms=(), after=()):
    rows, width = pieces[0].shape
    n_cols = w_down.shape[0]
    total = 2 * rows
    n_gate, n_x = n_cols // cols, width // x_cols

    def kernel(y0, y1, wd, g0, g1, u0, u1, wg, wu, *refs):
        o_gate, o_up, o_z, o_x0, o_x1 = refs[len(terms):len(terms) + 5]
        s_gate, s_up, held, sem = refs[-4:]
        step = pl.program_id(0)

        def fetch(tile):
            at = pl.ds(pl.multiple_of(tile * x_cols, x_cols), x_cols)
            slot = lax.rem(tile, 2)
            return [pltpu.make_async_copy(w.at[at], held.at[slot, k], sem.at[slot, k]) for k, w in enumerate((wg, wu))]

        @pl.when(step == n_gate - 1)
        def _():
            for copy in fetch(0):
                copy.start()

        def add_terms():
            if terms:
                refs[7][...] = (refs[0][...].astype(F32) + refs[1][...].astype(F32)).astype(BF16)

        @pl.when(step < n_gate)
        def _():
            add_terms()
            at = pl.ds(pl.multiple_of(step * cols, cols), cols)
            grad_y = jnp.concatenate([y0[...], y1[...]], axis=0)
            grad_h = lax.dot_general(grad_y, wd[...], NT, preferred_element_type=F32)
            gate_f = jnp.concatenate([g0[...], g1[...]], axis=0).astype(F32)
            up_f = jnp.concatenate([u0[...], u1[...]], axis=0).astype(F32)
            sig = jax.nn.sigmoid(gate_f)
            act = gate_f * sig
            d_up = (grad_h * act).astype(BF16)
            d_gate = (grad_h * up_f * (sig * (1.0 + gate_f * (1.0 - sig)))).astype(BF16)
            o_z[...] = (act * up_f).astype(BF16)
            o_up[...] = d_up
            o_gate[...] = d_gate
            s_up[:, at] = d_up
            s_gate[:, at] = d_gate

        @pl.when(step >= n_gate)
        def _():
            tile = step - n_gate

            @pl.when(tile + 1 < n_x)
            def _():
                for copy in fetch(tile + 1):
                    copy.start()

            for copy in fetch(tile):
                copy.wait()
            add_terms()
            slot = lax.rem(tile, 2)
            part = (lax.dot_general(s_gate[...], held[slot, 0], NT, preferred_element_type=F32)
                    + lax.dot_general(s_up[...], held[slot, 1], NT, preferred_element_type=F32)).astype(BF16)
            o_x0[...] = part[:rows]
            o_x1[...] = part[rows:]

    first = lambda j: jnp.minimum(j, n_gate - 1)
    second = lambda j: jnp.maximum(j - n_gate, 0)
    whole = pl.BlockSpec((rows, width), lambda j, o: (0, 0))
    tiles = [pl.BlockSpec((rows, cols), functools.partial(lambda s, j, o: (s(o), first(j)), s)) for s in starts]
    w_x = pl.BlockSpec(memory_space=pl.ANY)
    out = pl.BlockSpec((total, cols), lambda j, o: (0, first(j)))
    out_x = pl.BlockSpec((rows, x_cols), lambda j, o: (0, second(j)))
    sums = [pl.BlockSpec((t.shape[0] // 8, width), lambda j, o: (jnp.minimum(j, 7), 0)) for t in terms]
    return call(
        kernel, (n_gate + n_x,),
        [whole, whole, pl.BlockSpec((cols, width), lambda j, o: (first(j), 0)), *tiles, *tiles, w_x, w_x, *sums],
        [out] * 3 + [out_x] * 2 + sums[:1],
        [jax.ShapeDtypeStruct((total, n_cols), BF16)] * 3 + [jax.ShapeDtypeStruct((rows, width), BF16)] * 2
        + [jax.ShapeDtypeStruct(t.shape, BF16) for t in terms[:1]],
        6 * total * width * n_cols, 2 * n_cols * (3 * width + 5 * total),
        scratch=[pltpu.VMEM((total, n_cols), BF16)] * 2
        + [pltpu.VMEM((2, 2, x_cols, n_cols), BF16), pltpu.SemaphoreType.DMA((2, 2))], after=after, offs=offs,
    )(*pieces, w_down, u_gate, u_gate, u_up, u_up, w_gate, w_up, *terms)


def gw_in(x_parts, gates, ups, span, prev, rows, cols, norm=(), norm_size=0, after=()):
    width = x_parts[0].shape[1]
    n_tok = sum(x.shape[0] for x in x_parts)
    n_cols = gates[0].shape[1]
    half = gates[1].shape[0] // 2
    start, count = span[0] // rows, (span[1] - span[0]) // rows

    def kernel(*refs):
        x_own, x_par, x_acr, x_dia = (r[...] for r in refs[:4])
        x = [jnp.concatenate([x_own, x_par], axis=0)]
        x += [jnp.concatenate([x_acr[c * half:(c + 1) * half], x_dia[c * half:(c + 1) * half]], axis=0) for c in range(2)]
        for ds, out in ((refs[4:7], refs[-2]), (refs[7:10], refs[-1])):
            total = None
            for a, d in zip(x, ds):
                term = lax.dot_general(a, d[...], TN, preferred_element_type=F32)
                total = term if total is None else total + term
            out[...] = total
        if norm:
            some = norm_rows(*refs[10:16])
            refs[16][...] = some
            refs[17][...] = some

    in_specs = [pl.BlockSpec((x.shape[0], rows), lambda i, j: (0, start + i)) for x in x_parts]
    in_specs += [pl.BlockSpec((d.shape[0], cols), lambda i, j: (0, j)) for d in (*gates, *ups)]
    args = [*x_parts, *gates, *ups]
    aliases = None
    if prev is not None:
        in_specs += [pl.BlockSpec(memory_space=pl.ANY)] * 2
        args += list(prev)
        aliases = {10: 0, 11: 1}
    more_specs, more = [], []
    if norm:
        some_rows = pl.BlockSpec((norm_size * cols // n_cols, width), lambda i, j: (j, 0))
        in_specs += [some_rows] * 4 + [pl.BlockSpec((width,), lambda i, j: (0,)), some_rows]
        args += list(norm)
        more_specs = [some_rows] * 2
        more = [jax.ShapeDtypeStruct((norm_size, width), BF16), jax.ShapeDtypeStruct(norm[3].shape, BF16)]
    return call(
        kernel, (count, n_cols // cols), in_specs,
        more_specs + [pl.BlockSpec((rows, cols), lambda i, j: (start + i, j))] * 2,
        more + [jax.ShapeDtypeStruct((width, n_cols), F32)] * 2,
        4 * n_tok * (span[1] - span[0]) * n_cols, 8 * (span[1] - span[0]) * n_cols, after=after, aliases=aliases,
    )(*args)


def gw_down(zs, y_pairs, rows, cols, after=()):
    n_rows = zs[0].shape[1]
    width = y_pairs[0][0].shape[1]
    flat = [y for pair in y_pairs for y in pair]
    n_tok = sum(z.shape[0] for z in zs)

    def kernel(z0, z1, z2, a0, b0, a1, b1, a2, b2, out):
        total = None
        for z, a, b in ((z0, a0, b0), (z1, a1, b1), (z2, a2, b2)):
            y = jnp.concatenate([a[...], b[...]], axis=0)
            term = lax.dot_general(z[...], y, TN, preferred_element_type=F32)
            total = term if total is None else total + term
        out[...] = total

    return call(
        kernel, (n_rows // rows, width // cols),
        [pl.BlockSpec((z.shape[0], rows), lambda i, j: (0, i)) for z in zs]
        + [pl.BlockSpec((y.shape[0], cols), lambda i, j: (0, j)) for y in flat],
        pl.BlockSpec((rows, cols), lambda i, j: (i, j)),
        jax.ShapeDtypeStruct((n_rows, width), F32),
        2 * n_tok * width * n_rows, 4 * width * n_rows, after=after,
    )(*zs, *flat)


def head_rows(x, start, rows, block=128, after=()):
    width = x.shape[1]
    first = start // block

    def kernel(src, out):
        out[...] = src[...]

    return call(
        kernel, (rows // block,), [pl.BlockSpec((block, width), lambda i: (first + i, 0))],
        pl.BlockSpec((block, width), lambda i: (i, 0)), jax.ShapeDtypeStruct((rows, width), x.dtype),
        rows * width, rows * width * 4, after=after,
    )(x)


def norm_rows(p0, p1, p2, x_in, gamma, grad_res):
    grad_x = (p0[...].astype(F32) + p1[...].astype(F32) + p2[...].astype(F32)).astype(BF16).astype(F32)
    xin_f = x_in[...].astype(F32)
    inv_rms = lax.rsqrt(jnp.mean(xin_f * xin_f, axis=-1, keepdims=True) + NORM_EPS)
    scaled = grad_x * gamma[...].astype(F32).reshape(1, -1)
    proj_mean = jnp.mean(scaled * xin_f, axis=-1, keepdims=True)
    return (grad_res[...].astype(F32) + inv_rms * (scaled - xin_f * (inv_rms * inv_rms) * proj_mean)).astype(BF16)


def norm_chunk(parts, starts, rows, first_row, x_in, gamma, grad_res, prev, cuts, block=128, after=()):
    width = x_in.shape[1]
    n_cuts = len(cuts)
    edges = [sum(cuts[:k]) // block for k in range(n_cuts + 1)]

    def kernel(p0, p1, p2, xin, gam, res, *outs):
        outs = outs[-1 - n_cuts:]
        out = norm_rows(p0, p1, p2, xin, gam, res)
        outs[-1][...] = out
        for k in range(n_cuts):
            @pl.when((pl.program_id(0) >= edges[k]) & (pl.program_id(0) < edges[k + 1]))
            def _(k=k):
                outs[k][...] = out

    first = first_row // block
    at = lambda s: pl.BlockSpec((block, width), lambda i: (s + i, 0))
    cut = lambda k: pl.BlockSpec((block, width), lambda i: (jnp.clip(i - edges[k], 0, edges[k + 1] - edges[k] - 1), 0))
    in_specs = [at(s // block) for s in starts] + [at(first), pl.BlockSpec((width,), lambda i: (0,)), at(first)]
    args = [*parts, x_in, gamma, grad_res]
    aliases = None
    if prev is not None:
        in_specs.append(pl.BlockSpec(memory_space=pl.ANY))
        args.append(prev)
        aliases = {len(in_specs) - 1: n_cuts}
    return call(
        kernel, (rows // block,), in_specs, [cut(k) for k in range(n_cuts)] + [at(first)],
        [jax.ShapeDtypeStruct((c, width), BF16) for c in cuts] + [jax.ShapeDtypeStruct(x_in.shape, BF16)],
        rows * width * 20, rows * width * 14, after=after, aliases=aliases,
    )(*args)


def grad_attention(pieces, at_rows, blocks, w_out, offs, n_tok, group=2, after=()):
    n_cols, width = w_out.shape
    n = len(pieces)
    size = n_tok // 8

    def kernel(offs_ref, *refs):
        srcs, w, out, held, held_w, made, in_sem, w_sem, out_sem = *(refs[:n],), *refs[n:]
        loads = [pltpu.make_async_copy(w, held_w, w_sem.at[0])]
        loads += [pltpu.make_async_copy(srcs[q].at[pl.ds(at_rows[q] * size, size)], held.at[q], in_sem.at[q]) for q in range(n)]
        for load in loads[:1 + group]:
            load.start()
        loads[0].wait()
        stores = []
        for first in range(0, n, group):
            for q in range(first, first + group):
                loads[1 + q].wait()
            if first == 0:
                for load in loads[1 + group:]:
                    load.start()
            lhs = held[first:first + group].reshape(group * size, width)
            part = lax.dot_general(lhs, held_w[...], NT, preferred_element_type=F32).astype(BF16)
            made[first:first + group] = part.reshape(group, size, n_cols)
            for q in range(first, first + group):
                row = pl.multiple_of(blocks[q](offs_ref) * size, size)
                stores.append(pltpu.make_async_copy(made.at[q], out.at[pl.ds(row, size)], out_sem.at[q]))
                stores[-1].start()
        for store in stores:
            store.wait()

    anywhere = pl.BlockSpec(memory_space=pl.ANY)
    return call(
        kernel, (1,), [anywhere] * (n + 1), anywhere, jax.ShapeDtypeStruct((n_tok, n_cols), BF16),
        2 * n * size * width * n_cols, 2 * width * n_cols, after=after, offs=offs, keep_offs=True,
        scratch=[pltpu.VMEM((n, size, width), BF16), pltpu.VMEM((n_cols, width), BF16), pltpu.VMEM((n, size, n_cols), BF16),
                 pltpu.SemaphoreType.DMA((n,)), pltpu.SemaphoreType.DMA((1,)), pltpu.SemaphoreType.DMA((n,))],
    )(*pieces, w_out)


def out_grads(pieces, blocks, todo, attn_out, w_out, offs, d_attn, cols, after=()):
    n_tok, n_rows = attn_out.shape
    width = w_out.shape[1]
    n = len(pieces)
    sizes = [p.shape[0] for p in pieces]
    left = sum(sizes[q] for q in todo)
    last = width // cols - 1

    def kernel(offs_ref, *refs):
        srcs, attn, w = refs[:n], refs[n:2 * n], refs[2 * n]
        o_attn, o_w, acc, done, sem = refs[-5:]
        step = pl.program_id(0)
        term = lax.dot_general(jnp.concatenate([srcs[q][...] for q in todo], axis=0), w[...], NT, preferred_element_type=F32)
        lhs = jnp.concatenate([a[...] for a in attn], axis=0)
        rhs = jnp.concatenate([src[...] for src in srcs], axis=0)
        o_w[...] = lax.dot_general(lhs, rhs, TN, preferred_element_type=F32)

        @pl.when(step == 0)
        def _():
            acc[...] = term

        @pl.when((step > 0) & (step < last))
        def _():
            acc[...] += term

        @pl.when(step == last)
        def _():
            done[...] = (acc[...] + term).astype(BF16)
            copies, first = [], 0
            for k, q in enumerate(todo):
                row = pl.multiple_of(blocks[q](offs_ref) * sizes[q], sizes[q])
                copies.append(pltpu.make_async_copy(
                    done.at[pl.ds(first, sizes[q])], o_attn.at[pl.ds(row, sizes[q])], sem.at[k]))
                copies[-1].start()
                first += sizes[q]
            for copy in copies:
                copy.wait()

    in_specs = [pl.BlockSpec((r, cols), lambda j, o: (0, j)) for r in sizes]
    in_specs += [pl.BlockSpec((r, n_rows), functools.partial(lambda m, j, o: (m(o), 0), m)) for r, m in zip(sizes, blocks)]
    in_specs += [pl.BlockSpec((n_rows, cols), lambda j, o: (0, j)), pl.BlockSpec(memory_space=pl.ANY)]
    return call(
        kernel, (width // cols,), in_specs,
        [pl.BlockSpec(memory_space=pl.ANY), pl.BlockSpec((n_rows, cols), lambda j, o: (0, j))],
        [jax.ShapeDtypeStruct((n_tok, n_rows), BF16), jax.ShapeDtypeStruct((n_rows, width), F32)],
        2 * (n_tok + left) * width * n_rows, 4 * width * n_rows, after=after, offs=offs, keep_offs=True,
        aliases={2 * n + 1: 0},
        scratch=[pltpu.VMEM((left, n_rows), F32), pltpu.VMEM((left, n_rows), BF16), pltpu.SemaphoreType.DMA((len(todo),))],
    )(*pieces, *([attn_out] * n), w_out, d_attn)


def solution(mesh):
    token_spec = P(("dp", "tp"), None)
    split_cols = P("dp", "tp")
    weight_cols = P(None, "tp")
    weight_rows = P("tp", None)
    partner = [(i, i ^ 1) for i in range(4)]
    across = [(i, i ^ 2) for i in range(4)]

    def swap(x):
        return lax.ppermute(x, "tp", partner)

    def send(x):
        return lax.ppermute(x, "tp", across)

    def backward(x_norm, grad_y, u_gate, u_up, w_gate, w_up, w_down, x_in, gamma, grad_res, attn_out, w_out):
        own, width = grad_y.shape
        half = own // 2
        n_tok = u_gate.shape[0]
        offs = lax.axis_index("tp") ^ jnp.arange(4, dtype=jnp.int32)
        gain = gamma
        of = lambda p, c: (lambda o: 2 * o[p] + c)
        weights = (w_down, w_gate, w_up, u_gate, u_up, offs)

        y_par = swap(grad_y)
        head0 = head_rows(grad_y, 0, half)
        head1 = head_rows(grad_y, half, half, after=(head0,))
        y_acr = [send(head0), send(head1)]
        y_dia = [swap(y_acr[c]) for c in range(2)]
        x_par = swap(x_norm)
        x_acr = send(x_norm)
        x_dia = swap(x_acr)
        x_parts = (x_norm, x_par, x_acr, x_dia)

        g_l, u_l, z_l, dx_own, dx_par = input_grads(
            (grad_y, y_par), (lambda o: o[0], lambda o: o[1]), *weights, 256, 512, after=(head1,))
        dx_sib = swap(dx_par)
        gates, ups, zs = [g_l], [u_l], [z_l]
        last, terms, both = dx_own, (), []
        for c in range(2):
            g, u, z, to_acr, to_dia, *summed = input_grads(
                (y_acr[c], y_dia[c]), (of(2, c), of(3, c)), *weights, 512, 512, terms=terms, after=(last,))
            both += summed
            last, terms = to_acr, (to_acr, swap(to_dia))
            gates.append(g)
            ups.append(u)
            zs.append(z)
        both.append((terms[0].astype(F32) + terms[1].astype(F32)).astype(BF16))
        rs = [send(both[c]) for c in range(2)]

        gwd = gw_down(zs, ((grad_y, y_par), (y_acr[0], y_dia[0]), (y_acr[1], y_dia[1])), 1024, 1024, after=(last,))
        third = width // 3
        norm = (x_in, gain, grad_res)
        ds0, ds, *gw = gw_in(x_parts, gates, ups, (0, third), None, 1024, 512,
                             norm=(dx_own, dx_sib, rs[0], *norm), norm_size=half, after=(gwd, both[1]))
        s_acr0, s_par0 = send(ds0), swap(ds0)
        gw = gw_in(x_parts, gates, ups, (third, 2 * third), gw, 1024, 512, after=(ds0,))
        ds1, ds = norm_chunk((dx_own, dx_sib, rs[1]), (half, half, 0), half, half, *norm, ds, (half,), after=(gw[0],))
        s_acr1, s_par1 = send(ds1), swap(ds1)
        gwg, gwu = gw_in(x_parts, gates, ups, (2 * third, width), gw, 1024, 512, after=(ds1,))
        s_dia0, s_dia1 = swap(s_acr0), swap(s_acr1)

        d_attn = grad_attention((ds, ds, s_par0, s_par1, s_acr0, s_dia0), (0, 1, 0, 0, 0, 0),
                                (of(0, 0), of(0, 1), of(1, 0), of(1, 1), of(2, 0), of(3, 0)), w_out, offs, n_tok, after=(gwg,))
        d_attn, gwo = out_grads((ds, s_par0, s_par1, s_acr0, s_dia0, s_acr1, s_dia1),
                                (lambda o: o[0], of(1, 0), of(1, 1), of(2, 0), of(3, 0), of(2, 1), of(3, 1)), (5, 6),
                                attn_out, w_out, offs, d_attn, 512)
        return ds, d_attn, gwg, gwu, gwd, gwo

    return jax.shard_map(
        backward,
        mesh=mesh,
        in_specs=(token_spec, token_spec, split_cols, split_cols, weight_cols, weight_cols, weight_rows,
                  token_spec, P(None), token_spec, split_cols, weight_rows),
        out_specs=(token_spec, split_cols, split_cols, split_cols, token_spec, token_spec),
        check_vma=False,
    )
```

```python
import functools

import jax
import jax.numpy as jnp
from jax import lax
from jax.experimental import pallas as pl
from jax.experimental.pallas import tpu as pltpu
from jax.sharding import PartitionSpec as P


NORM_EPS = 1e-5
F32 = jnp.float32
BF16 = jnp.bfloat16
NT = (((1,), (1,)), ((), ()))
TN = (((0,), (0,)), ((), ()))
VMEM_LIMIT = 67043328


def call(kernel, grid, in_specs, out_specs, out_shape, flops, nbytes, scratch=(), after=(), offs=None, aliases=None, keep_offs=False):
    n_in, n_after = len(in_specs), len(after)
    n_pre = 0 if offs is None else 1

    def body(*refs):
        pre, refs = refs[:n_pre], refs[n_pre:]
        kernel(*(pre if keep_offs else ()), *refs[:n_in], *refs[n_in + n_after:])

    def run(*args):
        pre = () if offs is None else (offs,)
        return launch(pre, args)

    def launch(pre, args):
        return pl.pallas_call(
            body,
            grid_spec=pltpu.PrefetchScalarGridSpec(
                num_scalar_prefetch=n_pre,
                grid=grid,
                in_specs=list(in_specs) + [pl.BlockSpec(memory_space=pl.ANY)] * n_after,
                out_specs=out_specs,
                scratch_shapes=list(scratch),
            ),
            out_shape=out_shape,
            input_output_aliases={n_pre + i: o for i, o in (aliases or {}).items()},
            compiler_params=pltpu.CompilerParams(
                vmem_limit_bytes=VMEM_LIMIT, dimension_semantics=("arbitrary",) * len(grid)
            ),
            cost_estimate=pl.CostEstimate(flops=flops, bytes_accessed=nbytes, transcendentals=0),
        )(*pre, *args, *after)

    return run


def input_grads(pieces, starts, w_down, w_gate, w_up, u_gate, u_up, offs, cols, x_cols, terms=(), after=()):
    rows, width = pieces[0].shape
    n_cols = w_down.shape[0]
    total = 2 * rows
    n_gate, n_x = n_cols // cols, width // x_cols

    def kernel(y0, y1, wd, g0, g1, u0, u1, wg, wu, *refs):
        o_gate, o_up, o_z, o_x0, o_x1 = refs[len(terms):len(terms) + 5]
        s_gate, s_up, held, sem = refs[-4:]
        step = pl.program_id(0)

        def fetch(tile):
            at = pl.ds(pl.multiple_of(tile * x_cols, x_cols), x_cols)
            slot = lax.rem(tile, 2)
            return [pltpu.make_async_copy(w.at[at], held.at[slot, k], sem.at[slot, k]) for k, w in enumerate((wg, wu))]

        @pl.when(step == n_gate - 1)
        def _():
            for copy in fetch(0):
                copy.start()

        def add_terms():
            if terms:
                refs[7][...] = (refs[0][...].astype(F32) + refs[1][...].astype(F32)).astype(BF16)

        @pl.when(step < n_gate)
        def _():
            add_terms()
            at = pl.ds(pl.multiple_of(step * cols, cols), cols)
            grad_y = jnp.concatenate([y0[...], y1[...]], axis=0)
            grad_h = lax.dot_general(grad_y, wd[...], NT, preferred_element_type=F32)
            gate_f = jnp.concatenate([g0[...], g1[...]], axis=0).astype(F32)
            up_f = jnp.concatenate([u0[...], u1[...]], axis=0).astype(F32)
            sig = jax.nn.sigmoid(gate_f)
            act = gate_f * sig
            d_up = (grad_h * act).astype(BF16)
            d_gate = (grad_h * up_f * (sig * (1.0 + gate_f * (1.0 - sig)))).astype(BF16)
            o_z[...] = (act * up_f).astype(BF16)
            o_up[...] = d_up
            o_gate[...] = d_gate
            s_up[:, at] = d_up
            s_gate[:, at] = d_gate

        @pl.when(step >= n_gate)
        def _():
            tile = step - n_gate

            @pl.when(tile + 1 < n_x)
            def _():
                for copy in fetch(tile + 1):
                    copy.start()

            for copy in fetch(tile):
                copy.wait()
            add_terms()
            slot = lax.rem(tile, 2)
            part = (lax.dot_general(s_gate[...], held[slot, 0], NT, preferred_element_type=F32)
                    + lax.dot_general(s_up[...], held[slot, 1], NT, preferred_element_type=F32)).astype(BF16)
            o_x0[...] = part[:rows]
            o_x1[...] = part[rows:]

    first = lambda j: jnp.minimum(j, n_gate - 1)
    second = lambda j: jnp.maximum(j - n_gate, 0)
    whole = pl.BlockSpec((rows, width), lambda j, o: (0, 0))
    tiles = [pl.BlockSpec((rows, cols), functools.partial(lambda s, j, o: (s(o), first(j)), s)) for s in starts]
    w_x = pl.BlockSpec(memory_space=pl.ANY)
    out = pl.BlockSpec((total, cols), lambda j, o: (0, first(j)))
    out_x = pl.BlockSpec((rows, x_cols), lambda j, o: (0, second(j)))
    sums = [pl.BlockSpec((t.shape[0] // 8, width), lambda j, o: (jnp.minimum(j, 7), 0)) for t in terms]
    return call(
        kernel, (n_gate + n_x,),
        [whole, whole, pl.BlockSpec((cols, width), lambda j, o: (first(j), 0)), *tiles, *tiles, w_x, w_x, *sums],
        [out] * 3 + [out_x] * 2 + sums[:1],
        [jax.ShapeDtypeStruct((total, n_cols), BF16)] * 3 + [jax.ShapeDtypeStruct((rows, width), BF16)] * 2
        + [jax.ShapeDtypeStruct(t.shape, BF16) for t in terms[:1]],
        6 * total * width * n_cols, 2 * n_cols * (3 * width + 5 * total),
        scratch=[pltpu.VMEM((total, n_cols), BF16)] * 2
        + [pltpu.VMEM((2, 2, x_cols, n_cols), BF16), pltpu.SemaphoreType.DMA((2, 2))], after=after, offs=offs,
    )(*pieces, w_down, u_gate, u_gate, u_up, u_up, w_gate, w_up, *terms)


def gw_in(x_parts, gates, ups, span, prev, rows, cols, norm=(), norm_size=0, after=()):
    width = x_parts[0].shape[1]
    n_tok = sum(x.shape[0] for x in x_parts)
    n_cols = gates[0].shape[1]
    half = gates[1].shape[0] // 2
    start, count = span[0] // rows, (span[1] - span[0]) // rows

    def kernel(*refs):
        x_own, x_par, x_acr, x_dia = (r[...] for r in refs[:4])
        x = [jnp.concatenate([x_own, x_par], axis=0)]
        x += [jnp.concatenate([x_acr[c * half:(c + 1) * half], x_dia[c * half:(c + 1) * half]], axis=0) for c in range(2)]
        for ds, out in ((refs[4:7], refs[-2]), (refs[7:10], refs[-1])):
            total = None
            for a, d in zip(x, ds):
                term = lax.dot_general(a, d[...], TN, preferred_element_type=F32)
                total = term if total is None else total + term
            out[...] = total
        if norm:
            some = norm_rows(*refs[10:16])
            refs[16][...] = some
            refs[17][...] = some

    in_specs = [pl.BlockSpec((x.shape[0], rows), lambda i, j: (0, start + i)) for x in x_parts]
    in_specs += [pl.BlockSpec((d.shape[0], cols), lambda i, j: (0, j)) for d in (*gates, *ups)]
    args = [*x_parts, *gates, *ups]
    aliases = None
    if prev is not None:
        in_specs += [pl.BlockSpec(memory_space=pl.ANY)] * 2
        args += list(prev)
        aliases = {10: 0, 11: 1}
    more_specs, more = [], []
    if norm:
        some_rows = pl.BlockSpec((norm_size * cols // n_cols, width), lambda i, j: (j, 0))
        in_specs += [some_rows] * 4 + [pl.BlockSpec((width,), lambda i, j: (0,)), some_rows]
        args += list(norm)
        more_specs = [some_rows] * 2
        more = [jax.ShapeDtypeStruct((norm_size, width), BF16), jax.ShapeDtypeStruct(norm[3].shape, BF16)]
    return call(
        kernel, (count, n_cols // cols), in_specs,
        more_specs + [pl.BlockSpec((rows, cols), lambda i, j: (start + i, j))] * 2,
        more + [jax.ShapeDtypeStruct((width, n_cols), F32)] * 2,
        4 * n_tok * (span[1] - span[0]) * n_cols, 8 * (span[1] - span[0]) * n_cols, after=after, aliases=aliases,
    )(*args)


def gw_down(zs, y_pairs, rows, cols, after=()):
    n_rows = zs[0].shape[1]
    width = y_pairs[0][0].shape[1]
    flat = [y for pair in y_pairs for y in pair]
    n_tok = sum(z.shape[0] for z in zs)

    def kernel(z0, z1, z2, a0, b0, a1, b1, a2, b2, out):
        total = None
        for z, a, b in ((z0, a0, b0), (z1, a1, b1), (z2, a2, b2)):
            y = jnp.concatenate([a[...], b[...]], axis=0)
            term = lax.dot_general(z[...], y, TN, preferred_element_type=F32)
            total = term if total is None else total + term
        out[...] = total

    return call(
        kernel, (n_rows // rows, width // cols),
        [pl.BlockSpec((z.shape[0], rows), lambda i, j: (0, i)) for z in zs]
        + [pl.BlockSpec((y.shape[0], cols), lambda i, j: (0, j)) for y in flat],
        pl.BlockSpec((rows, cols), lambda i, j: (i, j)),
        jax.ShapeDtypeStruct((n_rows, width), F32),
        2 * n_tok * width * n_rows, 4 * width * n_rows, after=after,
    )(*zs, *flat)


def head_rows(x, start, rows, block=128, after=()):
    width = x.shape[1]
    first = start // block

    def kernel(src, out):
        out[...] = src[...]

    return call(
        kernel, (rows // block,), [pl.BlockSpec((block, width), lambda i: (first + i, 0))],
        pl.BlockSpec((block, width), lambda i: (i, 0)), jax.ShapeDtypeStruct((rows, width), x.dtype),
        rows * width, rows * width * 4, after=after,
    )(x)


def norm_rows(p0, p1, p2, x_in, gamma, grad_res):
    grad_x = (p0[...].astype(F32) + p1[...].astype(F32) + p2[...].astype(F32)).astype(BF16).astype(F32)
    xin_f = x_in[...].astype(F32)
    inv_rms = lax.rsqrt(jnp.mean(xin_f * xin_f, axis=-1, keepdims=True) + NORM_EPS)
    scaled = grad_x * gamma[...].astype(F32).reshape(1, -1)
    proj_mean = jnp.mean(scaled * xin_f, axis=-1, keepdims=True)
    return (grad_res[...].astype(F32) + inv_rms * (scaled - xin_f * (inv_rms * inv_rms) * proj_mean)).astype(BF16)


def norm_chunk(parts, starts, rows, first_row, x_in, gamma, grad_res, prev, block=64, after=()):
    width = x_in.shape[1]
    n_blocks = rows // block
    firsts = (*starts, first_row, first_row)

    def kernel(p0, p1, p2, xin, res, gam, _, o_chunk, o_full, held, made, in_sem, out_sem):
        srcs = (p0, p1, p2, xin, res)

        def loads(b):
            return [pltpu.make_async_copy(src.at[pl.ds(pl.multiple_of(first + b * block, block), block)], held.at[b, k], in_sem.at[b, k])
                    for k, (src, first) in enumerate(zip(srcs, firsts))]

        for b in range(n_blocks):
            for copy in loads(b):
                copy.start()

        def store(b):
            at = pl.multiple_of(b * block, block)
            return [pltpu.make_async_copy(made.at[b], o_chunk.at[pl.ds(at, block)], out_sem.at[b, 0]),
                    pltpu.make_async_copy(made.at[b], o_full.at[pl.ds(first_row + at, block)], out_sem.at[b, 1])]

        def step(b, _):
            for copy in loads(b):
                copy.wait()
            made[b] = norm_rows(held[b, 0], held[b, 1], held[b, 2], held[b, 3], gam, held[b, 4])
            for copy in store(b):
                copy.start()
            return 0

        lax.fori_loop(0, n_blocks, step, 0)
        for b in range(n_blocks):
            for copy in store(b):
                copy.wait()

    anywhere = pl.BlockSpec(memory_space=pl.ANY)
    return call(
        kernel, (1,), [anywhere] * 5 + [pl.BlockSpec((width,), lambda i: (0,)), anywhere], [anywhere] * 2,
        [jax.ShapeDtypeStruct((rows, width), BF16), jax.ShapeDtypeStruct(x_in.shape, BF16)],
        rows * width * 20, rows * width * 14, after=after, aliases={6: 1},
        scratch=[pltpu.VMEM((n_blocks, 5, block, width), BF16), pltpu.VMEM((n_blocks, block, width), BF16),
                 pltpu.SemaphoreType.DMA((n_blocks, 5)), pltpu.SemaphoreType.DMA((n_blocks, 2))],
    )(*parts, x_in, grad_res, gamma, prev)


def grad_attention(pieces, at_rows, blocks, w_out, offs, n_tok, group=2, after=()):
    n_cols, width = w_out.shape
    n = len(pieces)
    size = n_tok // 8

    def kernel(offs_ref, *refs):
        srcs, w, out, held, held_w, made, in_sem, w_sem, out_sem = *(refs[:n],), *refs[n:]
        loads = [pltpu.make_async_copy(w, held_w, w_sem.at[0])]
        loads += [pltpu.make_async_copy(srcs[q].at[pl.ds(at_rows[q] * size, size)], held.at[q], in_sem.at[q]) for q in range(n)]
        for load in loads[:1 + group]:
            load.start()
        loads[0].wait()
        stores = []
        for first in range(0, n, group):
            for q in range(first, first + group):
                loads[1 + q].wait()
            if first == 0:
                for load in loads[1 + group:]:
                    load.start()
            lhs = held[first:first + group].reshape(group * size, width)
            part = lax.dot_general(lhs, held_w[...], NT, preferred_element_type=F32).astype(BF16)
            made[first:first + group] = part.reshape(group, size, n_cols)
            for q in range(first, first + group):
                row = pl.multiple_of(blocks[q](offs_ref) * size, size)
                stores.append(pltpu.make_async_copy(made.at[q], out.at[pl.ds(row, size)], out_sem.at[q]))
                stores[-1].start()
        for store in stores:
            store.wait()

    anywhere = pl.BlockSpec(memory_space=pl.ANY)
    return call(
        kernel, (1,), [anywhere] * (n + 1), anywhere, jax.ShapeDtypeStruct((n_tok, n_cols), BF16),
        2 * n * size * width * n_cols, 2 * width * n_cols, after=after, offs=offs, keep_offs=True,
        scratch=[pltpu.VMEM((n, size, width), BF16), pltpu.VMEM((n_cols, width), BF16), pltpu.VMEM((n, size, n_cols), BF16),
                 pltpu.SemaphoreType.DMA((n,)), pltpu.SemaphoreType.DMA((1,)), pltpu.SemaphoreType.DMA((n,))],
    )(*pieces, w_out)


def out_grads(pieces, blocks, todo, attn_out, w_out, offs, d_attn, cols, after=()):
    n_tok, n_rows = attn_out.shape
    width = w_out.shape[1]
    n = len(pieces)
    sizes = [p.shape[0] for p in pieces]
    left = sum(sizes[q] for q in todo)
    last = width // cols - 1

    def kernel(offs_ref, *refs):
        srcs, attn, w = refs[:n], refs[n:2 * n], refs[2 * n]
        o_attn, o_w, acc, done, sem = refs[-5:]
        step = pl.program_id(0)
        term = lax.dot_general(jnp.concatenate([srcs[q][...] for q in todo], axis=0), w[...], NT, preferred_element_type=F32)
        lhs = jnp.concatenate([a[...] for a in attn], axis=0)
        rhs = jnp.concatenate([src[...] for src in srcs], axis=0)
        o_w[...] = lax.dot_general(lhs, rhs, TN, preferred_element_type=F32)

        @pl.when(step == 0)
        def _():
            acc[...] = term

        @pl.when((step > 0) & (step < last))
        def _():
            acc[...] += term

        @pl.when(step == last)
        def _():
            done[...] = (acc[...] + term).astype(BF16)
            copies, first = [], 0
            for k, q in enumerate(todo):
                row = pl.multiple_of(blocks[q](offs_ref) * sizes[q], sizes[q])
                copies.append(pltpu.make_async_copy(
                    done.at[pl.ds(first, sizes[q])], o_attn.at[pl.ds(row, sizes[q])], sem.at[k]))
                copies[-1].start()
                first += sizes[q]
            for copy in copies:
                copy.wait()

    in_specs = [pl.BlockSpec((r, cols), lambda j, o: (0, j)) for r in sizes]
    in_specs += [pl.BlockSpec((r, n_rows), functools.partial(lambda m, j, o: (m(o), 0), m)) for r, m in zip(sizes, blocks)]
    in_specs += [pl.BlockSpec((n_rows, cols), lambda j, o: (0, j)), pl.BlockSpec(memory_space=pl.ANY)]
    return call(
        kernel, (width // cols,), in_specs,
        [pl.BlockSpec(memory_space=pl.ANY), pl.BlockSpec((n_rows, cols), lambda j, o: (0, j))],
        [jax.ShapeDtypeStruct((n_tok, n_rows), BF16), jax.ShapeDtypeStruct((n_rows, width), F32)],
        2 * (n_tok + left) * width * n_rows, 4 * width * n_rows, after=after, offs=offs, keep_offs=True,
        aliases={2 * n + 1: 0},
        scratch=[pltpu.VMEM((left, n_rows), F32), pltpu.VMEM((left, n_rows), BF16), pltpu.SemaphoreType.DMA((len(todo),))],
    )(*pieces, *([attn_out] * n), w_out, d_attn)


def solution(mesh):
    token_spec = P(("dp", "tp"), None)
    split_cols = P("dp", "tp")
    weight_cols = P(None, "tp")
    weight_rows = P("tp", None)
    partner = [(i, i ^ 1) for i in range(4)]
    across = [(i, i ^ 2) for i in range(4)]

    def swap(x):
        return lax.ppermute(x, "tp", partner)

    def send(x):
        return lax.ppermute(x, "tp", across)

    def backward(x_norm, grad_y, u_gate, u_up, w_gate, w_up, w_down, x_in, gamma, grad_res, attn_out, w_out):
        own, width = grad_y.shape
        half = own // 2
        n_tok = u_gate.shape[0]
        offs = lax.axis_index("tp") ^ jnp.arange(4, dtype=jnp.int32)
        gain = gamma
        of = lambda p, c: (lambda o: 2 * o[p] + c)
        weights = (w_down, w_gate, w_up, u_gate, u_up, offs)

        y_par = swap(grad_y)
        head0 = head_rows(grad_y, 0, half)
        head1 = head_rows(grad_y, half, half, after=(head0,))
        y_acr = [send(head0), send(head1)]
        y_dia = [swap(y_acr[c]) for c in range(2)]
        x_par = swap(x_norm)
        x_acr = send(x_norm)
        x_dia = swap(x_acr)
        x_parts = (x_norm, x_par, x_acr, x_dia)

        g_l, u_l, z_l, dx_own, dx_par = input_grads(
            (grad_y, y_par), (lambda o: o[0], lambda o: o[1]), *weights, 256, 512, after=(head1,))
        dx_sib = swap(dx_par)
        gates, ups, zs = [g_l], [u_l], [z_l]
        last, terms, both = dx_own, (), []
        for c in range(2):
            g, u, z, to_acr, to_dia, *summed = input_grads(
                (y_acr[c], y_dia[c]), (of(2, c), of(3, c)), *weights, 512, 512, terms=terms, after=(last,))
            both += summed
            last, terms = to_acr, (to_acr, swap(to_dia))
            gates.append(g)
            ups.append(u)
            zs.append(z)
        both.append((terms[0].astype(F32) + terms[1].astype(F32)).astype(BF16))
        rs = [send(both[c]) for c in range(2)]

        gwd = gw_down(zs, ((grad_y, y_par), (y_acr[0], y_dia[0]), (y_acr[1], y_dia[1])), 1024, 1024, after=(last,))
        third = width // 3
        norm = (x_in, gain, grad_res)
        ds0, ds, *gw = gw_in(x_parts, gates, ups, (0, third), None, 1024, 512,
                             norm=(dx_own, dx_sib, rs[0], *norm), norm_size=half, after=(gwd, both[1]))
        s_acr0, s_par0 = send(ds0), swap(ds0)
        gw = gw_in(x_parts, gates, ups, (third, 2 * third), gw, 1024, 512, after=(ds0,))
        ds1, ds = norm_chunk((dx_own, dx_sib, rs[1]), (half, half, 0), half, half, *norm, ds, after=(gw[0],))
        s_acr1, s_par1 = send(ds1), swap(ds1)
        gwg, gwu = gw_in(x_parts, gates, ups, (2 * third, width), gw, 1024, 512, after=(ds1,))
        s_dia0, s_dia1 = swap(s_acr0), swap(s_acr1)

        d_attn = grad_attention((ds, ds, s_par0, s_par1, s_acr0, s_dia0), (0, 1, 0, 0, 0, 0),
                                (of(0, 0), of(0, 1), of(1, 0), of(1, 1), of(2, 0), of(3, 0)), w_out, offs, n_tok, after=(gwg,))
        d_attn, gwo = out_grads((ds, s_par0, s_par1, s_acr0, s_dia0, s_acr1, s_dia1),
                                (lambda o: o[0], of(1, 0), of(1, 1), of(2, 0), of(3, 0), of(2, 1), of(3, 1)), (5, 6),
                                attn_out, w_out, offs, d_attn, 512)
        return ds, d_attn, gwg, gwu, gwd, gwo

    return jax.shard_map(
        backward,
        mesh=mesh,
        in_specs=(token_spec, token_spec, split_cols, split_cols, weight_cols, weight_cols, weight_rows,
                  token_spec, P(None), token_spec, split_cols, weight_rows),
        out_specs=(token_spec, split_cols, split_cols, split_cols, token_spec, token_spec),
        check_vma=False,
    )
```
